32 devices in a mesh: row: 8 (over z, x), col: 4 (over y, core).
Axes of the slice: x: 2, y: 2, z: 4, core: 2. Of those that a mesh axis runs over, the one named last changes fastest.
Arguments:
- factor_u: float32 [1, 8, 2, 4, 512, 128], P(None, 'row', None, 'col'), may hold values from -6 to 6
- factor_v: float32 [1, 8, 2, 4, 512, 128], P(None, 'row', None, 'col'), may hold values from -6 to 6
- near_field: float32 [2, 512, 512], replicated, as said below
- sketch: float32 [2, 512, 128], replicated, may hold values from -6 to 6
- tile_ranks: int32 [3, 1, 8, 2, 4], P(None, None, None, None, 'col'), may hold values from 1 to 128, as said below
Outputs:
- out_u: float32 [1, 8, 2, 4, 512, 128], P(None, 'row', None, 'col')
- out_v: float32 [1, 8, 2, 4, 512, 128], P(None, 'row', None, 'col')
The draws below stay inside these ranges and needn't reach their ends.
Inputs may be any that keep to these rules, and one draw needn't show every extreme that they name: tile_ranks[0] is at least 16 and equals 128 on every tile (i, i); tile_ranks[1] lies between tile_ranks[0] - tile_ranks[0] // 2 and tile_ranks[0] - max(1, tile_ranks[0] // 4); tile_ranks[2] is at least 1 and at most tile_ranks[1], and when tile_ranks[1] > 1 it is at most tile_ranks[1] - max(1, tile_ranks[1] // 4). The diagonal entries of near_field[0] and near_field[1] lie between 1 and 4.
All inputs are finite; a program needn't handle non-finite values.
Results may differ from the reference program's by a relative error of at most 0.0003.
Values sent between devices are 32-bit elements; how exact they have to be, the bound alone decides.
A program may use at most 64 MiB of HBM per device.

```python
import math
import jax
import jax.numpy as jnp
from jax import lax

TILE = 512
KMAX = 128
NS_STEPS = 3
TRD = 1
TCD = 2
N_ROW = 8
N_COL = 4


def draw_near_field(key, part):
    key_diagonal, key_spread = jax.random.split(jax.random.fold_in(key, 11))
    identity = jnp.eye(TILE, dtype=jnp.float32)
    diagonal = jnp.exp(jax.random.uniform(key_diagonal, (2, TILE), jnp.float32, 0.0, 1.3862943))
    spread = jax.random.normal(key_spread, (2, TILE, TILE), jnp.float32)
    spread = spread * (0.1 / jnp.sqrt(jnp.float32(TILE)))
    diagonal = jnp.clip(diagonal, 1.0, 4.0)
    return spread * (1.0 - identity) + diagonal[:, :, None] * identity


def draw_tile_ranks(key, part):
    row_count = TRD * N_ROW
    col_count = TCD * N_COL
    label_count = max(row_count, col_count)
    key_list = jax.random.split(jax.random.fold_in(key, 29), 5)
    groups = jax.random.randint(key_list[0], (label_count,), 0, 4)
    heavy_pair = (groups[:row_count, None] == groups[None, :col_count]).astype(jnp.int32)
    base_rank = jax.random.randint(key_list[1], (row_count, col_count), KMAX // 8, KMAX // 2 + 1)
    extra_rank = jax.random.randint(key_list[2], (row_count, col_count), 0, KMAX // 2 + 1) * heavy_pair
    rank_first = jnp.minimum(base_rank + extra_rank, KMAX)
    on_diagonal = jnp.arange(row_count)[:, None] == jnp.arange(col_count)[None, :]
    rank_first = jnp.where(on_diagonal, KMAX, rank_first)
    low_first = jnp.maximum(1, rank_first // 4)
    rank_second = rank_first - jax.random.randint(key_list[3], (row_count, col_count), low_first, rank_first // 2 + 1)
    low_second = jnp.maximum(1, rank_second // 4)
    high_second = jnp.maximum(low_second, rank_second // 2)
    rank_third = jnp.maximum(1, rank_second - jax.random.randint(key_list[4], (row_count, col_count), low_second, high_second + 1))
    stacked = jnp.stack([rank_first, rank_second, rank_third]).astype(jnp.int32)
    return stacked.reshape(3, TRD, N_ROW, TCD, N_COL)


def steps_of(stream_key, shape, pieces, low, top_value):
    def one(position, blocks):
        steps = jax.random.uniform(jax.random.fold_in(jax.random.fold_in(stream_key, 6), position), (blocks,), jnp.float32, low / len(pieces), top_value / len(pieces))
        return jnp.repeat(jnp.exp(steps), shape[position] // blocks).reshape((-1,) + (1,) * (len(shape) - position - 1))

    factor_of = one(*pieces[0])
    for cut in pieces[1:]:
        factor_of = factor_of * one(*cut)
    return factor_of


def normal_values(stream_key, extent, scale, bound, cuts=(), kind=jnp.bfloat16):
    gain = steps_of(stream_key, extent, cuts, -0.22, 0.18) if cuts else 1.0
    drawn = jax.random.normal(stream_key, extent, jnp.float32) * scale * gain
    return jnp.minimum(jnp.maximum(drawn, -bound), bound).astype(kind)


def setup_inputs(seed: int = 0) -> dict:
    splits = jax.random.split(jax.random.key(seed), 6)
    factor_u = normal_values(splits[0], (TRD, N_ROW, TCD, N_COL, TILE, KMAX), 1.0, 6.0, ((1, 8), (3, 4)), jnp.float32)
    factor_v = normal_values(splits[1], (TRD, N_ROW, TCD, N_COL, TILE, KMAX), 1.0, 6.0, ((1, 8), (3, 4)), jnp.float32)
    near_field = draw_near_field(jax.random.fold_in(splits[5], 71), 0)
    sketch = normal_values(splits[3], (2, TILE, KMAX), 1.0, 6.0, (), jnp.float32)
    tile_ranks = draw_tile_ranks(jax.random.fold_in(splits[5], 71), 0)
    return {"factor_u": factor_u, "factor_v": factor_v, "near_field": near_field, "sketch": sketch, "tile_ranks": tile_ranks}


highest = lax.Precision.HIGHEST

def rank_keep(ranks, width):
    return jnp.arange(width, dtype=jnp.int32) < ranks[..., None]

def orthonormal(basis, keeper):
    gram = jnp.einsum('...tk,...tl->...kl', basis, basis, precision=highest)
    unused = 1.0 - keeper.astype(basis.dtype)
    gram = gram + jnp.eye(basis.shape[-1], dtype=basis.dtype) * unused[..., None, :]
    factor = jnp.linalg.cholesky(gram)
    solved = jax.scipy.linalg.solve_triangular(factor, jnp.swapaxes(basis, -1, -2), lower=True)
    return jnp.swapaxes(solved, -1, -2)

def recompress(full_u, full_v, sketch_block, ranks):
    root_order = math.sqrt(full_u.shape[-2])
    keeper = rank_keep(ranks, sketch_block.shape[-1])
    projected = jnp.einsum('...tq,tk->...qk', full_v, sketch_block, precision=highest)
    basis = jnp.einsum('...tq,...qk->...tk', full_u, projected, precision=highest)
    basis = basis * keeper[..., None, :].astype(basis.dtype)
    ortho = orthonormal(orthonormal(basis, keeper), keeper)
    backward = jnp.einsum('...tq,...tk->...qk', full_u, ortho, precision=highest)
    new_v = jnp.einsum('...tq,...qk->...tk', full_v, backward, precision=highest) / root_order
    return (ortho * root_order, new_v)

def update_tiles(cur_u, cur_v, low_u, low_v, up_u, up_v, sketch_block, ranks):
    far_weight = 1.0 / (8.0 * cur_u.shape[-2])
    core_block = far_weight * jnp.einsum('...tk,...tl->...kl', low_v, up_u, precision=highest)
    product_u = jnp.einsum('...tk,...kl->...tl', low_u, core_block, precision=highest)
    product_u = jnp.broadcast_to(product_u, cur_u.shape)
    full_u = jnp.concatenate([cur_u, -product_u], axis=-1)
    full_v = jnp.concatenate([cur_v, jnp.broadcast_to(up_v, cur_v.shape)], axis=-1)
    return (product_u, recompress(full_u, full_v, sketch_block, ranks))

def newton_inverse(pivot, start_inverse):
    inverse = jnp.diag(start_inverse)
    twice = 2.0 * jnp.eye(pivot.shape[0], dtype=pivot.dtype)
    for newton_step in range(NS_STEPS):
        inverse = jnp.dot(inverse, twice - jnp.dot(pivot, inverse, precision=highest), precision=highest)
    return inverse

def reference(factor_u, factor_v, near_field, sketch, tile_ranks):
    row_count = TRD * N_ROW
    col_count = TCD * N_COL
    cur_u = factor_u.reshape(row_count, col_count, TILE, KMAX)
    cur_v = factor_v.reshape(row_count, col_count, TILE, KMAX)
    all_ranks = tile_ranks.reshape(3, row_count, col_count)
    keeper = rank_keep(all_ranks[0], KMAX).astype(cur_u.dtype)[..., None, :]
    cur_u = cur_u * keeper
    cur_v = cur_v * keeper
    far_weight = 1.0 / (8.0 * TILE)
    tile_row = jnp.arange(row_count, dtype=jnp.int32)[:, None]
    tile_col = jnp.arange(col_count, dtype=jnp.int32)[None, :]
    pivot = near_field[0] + far_weight * jnp.dot(cur_u[0, 0], cur_v[0, 0].T, precision=highest)
    for panel in range(2):
        inverse = newton_inverse(pivot, 1.0 / jnp.diagonal(near_field[panel]))
        low_v = jnp.einsum('st,isk->itk', inverse, cur_v[:, panel], precision=highest)
        up_u = cur_u[panel]
        up_v = cur_v[panel]
        sketch_block = sketch[panel]

        def one_row(items):
            row_u, row_v, lead_u, lead_v, row_ranks = items
            unused_product, fresh_pair = update_tiles(row_u, row_v, lead_u[None], lead_v[None], up_u, up_v, sketch_block, row_ranks)
            return fresh_pair
        fresh_u, fresh_v = lax.map(one_row, (cur_u[panel + 1:], cur_v[panel + 1:], cur_u[panel + 1:, panel], low_v[panel + 1:], all_ranks[panel + 1, panel + 1:]))
        if panel == 0:
            core_block = far_weight * jnp.dot(low_v[1].T, cur_u[0, 1], precision=highest)
            product_one = jnp.dot(cur_u[1, 0], core_block, precision=highest)
            pivot = near_field[1] + far_weight * (jnp.dot(cur_u[1, 1], cur_v[1, 1].T, precision=highest) - jnp.dot(product_one, cur_v[0, 1].T, precision=highest))
        chosen = (tile_row > panel) & (tile_col > panel)
        if panel == 0:
            chosen = chosen & jnp.logical_not((tile_row == 1) & (tile_col == 1))
        chosen = chosen[panel + 1:, :, None, None]
        cur_u = cur_u.at[panel + 1:].set(jnp.where(chosen, fresh_u, cur_u[panel + 1:]))
        cur_v = cur_v.at[panel + 1:].set(jnp.where(chosen, fresh_v, cur_v[panel + 1:]))
        lower_here = tile_row[:, 0] > panel
        cur_v = cur_v.at[:, panel].set(jnp.where(lower_here[:, None, None], low_v, cur_v[:, panel]))
        cur_u = cur_u.at[panel, panel].set(jnp.zeros((TILE, KMAX), cur_u.dtype))
        cur_v = cur_v.at[panel, panel].set(jnp.zeros((TILE, KMAX), cur_v.dtype))
    shape_out = (TRD, N_ROW, TCD, N_COL, TILE, KMAX)
    return (cur_u.reshape(shape_out), cur_v.reshape(shape_out))
```

```python
import functools
import math

import jax
import jax.numpy as jnp
from jax import lax
from jax.experimental import pallas as pl
from jax.experimental.pallas import tpu as pltpu
from jax.sharding import PartitionSpec as P

NS_STEPS = 3
BLOCK = 16
F32 = jnp.float32
BF16 = jnp.bfloat16
VMEM_SPEC = pl.BlockSpec(memory_space=pltpu.VMEM)
SMEM_SPEC = pl.BlockSpec(memory_space=pltpu.SMEM)
MESH = pl.DeviceIdType.MESH


def split(x):
    high = x.astype(BF16)
    return high, (x - high.astype(F32)).astype(BF16)


def dot_pairs(a, b, contract_b=0):
    dims = (((1,), (contract_b,)), ((), ()))
    ah, al = a
    bh, bl = b
    mm = lambda p, q: lax.dot_general(p, q, dims, preferred_element_type=F32)
    return mm(ah, bh) + (mm(ah, bl) + mm(al, bh))


def dot(a, b):
    return dot_pairs(split(a), split(b))


def dot_nt(a, b):
    return dot_pairs(split(a), split(b), 1)


def dot_tn(a, b):
    return dot_pairs(split(a.T), split(b))


def apply_inverse(matrix, scale, w):
    pair = split(matrix)

    def step(level, x):
        if level == 0:
            return scale * x
        y = step(level - 1, x)
        return step(level - 1, 2.0 * x - dot_pairs(pair, split(y)))

    return step(NS_STEPS, w)


def diagonal_inverse(near):
    n = near.shape[0]
    eye = lax.broadcasted_iota(jnp.int32, (n, n), 0) == lax.broadcasted_iota(jnp.int32, (n, n), 1)
    return 1.0 / jnp.sum(jnp.where(eye, near, 0.0), axis=1, keepdims=True)


def cholesky_inverse(grams, order):
    width = grams[0].shape[1]
    count = len(grams)
    a = [g[:order] for g in grams]
    eye = (
        lax.broadcasted_iota(jnp.int32, (order, width), 0) == lax.broadcasted_iota(jnp.int32, (order, width), 1)
    ).astype(F32)
    w = [eye] * count
    done = [[] for _ in range(count)]
    start = 0
    while start < order:
        size = min(BLOCK, order - start)
        row_id = lax.broadcasted_iota(jnp.int32, (size, width), 0)
        r = [x[:size] for x in a]
        wr = [x[:size] for x in w]
        c = [[jnp.broadcast_to(x[:, start + j : start + j + 1], (size, width)) for j in range(size)] for x in r]
        scale = [jnp.ones((size, width), F32)] * count
        for k in range(size):
            for t in range(count):
                inv = lax.rsqrt(c[t][k][k : k + 1])
                m = jnp.where(row_id > k, c[t][k] * (inv * inv), 0.0)
                for j in range(k + 1, size):
                    c[t][j] = c[t][j] - m * c[t][j][k : k + 1]
                r[t] = r[t] - m * r[t][k : k + 1]
                wr[t] = wr[t] - m * wr[t][k : k + 1]
                scale[t] = jnp.where(row_id == k, inv, scale[t])
        for t in range(count):
            r[t] = r[t] * scale[t]
            wr[t] = wr[t] * scale[t]
            done[t].append(wr[t])
        end = start + size
        if end < order:
            for t in range(count):
                left = r[t].T[end:order]
                upd = jnp.dot(
                    left,
                    jnp.concatenate([r[t], wr[t]], axis=1),
                    precision=lax.Precision.HIGHEST,
                    preferred_element_type=F32,
                )
                a[t] = a[t][size:] - upd[:, :width]
                w[t] = w[t][size:] - upd[:, width:]
        start = end
    tail = width - order
    return [
        jnp.concatenate(d + ([jnp.zeros((tail, width), F32)] if tail else []), axis=0) for d in done
    ]


def orthonormal(bases, ranks, order):
    width = bases[0].shape[1]
    row = lax.broadcasted_iota(jnp.int32, (width, width), 0)
    col = lax.broadcasted_iota(jnp.int32, (width, width), 1)
    grams = []
    for basis, rank in zip(bases, ranks):
        gram = dot_tn(basis, basis)
        grams.append(gram + jnp.where((row == col) & (col >= rank), 1.0, 0.0))
    inverses = cholesky_inverse(grams, order)
    return [dot_nt(basis, inverse) for basis, inverse in zip(bases, inverses)]


def recompress(us, vs, wides, ups, sketch, ranks, order):
    height, width = us[0].shape
    root_order = math.sqrt(height)
    sk = split(sketch)
    bases = []
    for u, v, wide, up, rank in zip(us, vs, wides, ups, ranks):
        here = dot_pairs(split(v.T), sk)
        above = dot_pairs(split(up.T), sk)
        basis = dot(u, here) - dot(wide, above)
        keep = lax.broadcasted_iota(jnp.int32, (height, width), 1) < rank
        bases.append(jnp.where(keep, basis, 0.0))
    orthos = orthonormal(orthonormal(bases, ranks, order), ranks, order)
    out = []
    for u, v, wide, up, ortho in zip(us, vs, wides, ups, orthos):
        o = split(ortho)
        new_v = dot(v, dot_pairs(split(u.T), o)) - dot(up, dot_pairs(split(wide.T), o))
        out.append((ortho * root_order, new_v * (1.0 / root_order)))
    return out


class Tree:
    def __init__(self, root, edges):
        self.root = root
        self.edges = edges


def row_tree(n, source, r, c):
    levels = n // 2
    level, side, e = r // 2, (r + source) % 2, c % 2
    index = lambda l, s: 2 * l + (s + source) % 2
    spine = side == e
    edges = [
        (spine & (level + 1 < levels), (index(level + 1, e), c)),
        (jnp.logical_not(spine) & (level == 1 - e), (index(0, 1), c)),
        (spine & (level >= 1), (index(level, 1 - e), c)),
    ]
    return Tree((level == 0) & (side == 0), edges)


def col_tree(n, source, r, c):
    levels = n // 2
    level, side = c // 2, (c + source) % 2
    index = lambda l, s: 2 * l + (s + source) % 2
    edges = [
        ((side == 0) & (level + 1 < levels), (r, index(level + 1, 0))),
        (side == 0, (r, index(level, 1))),
    ]
    return Tree((level == 0) & (side == 0), edges)


class Piece:
    def __init__(self, tree, own, ref, send, recv, when=None):
        self.tree, self.own, self.ref, self.send, self.recv, self.when = tree, own, ref, send, recv, when

    def both(self, cond):
        return cond if self.when is None else cond & self.when

    def begin(self):
        @pl.when(self.both(self.tree.root))
        def _():
            pltpu.make_async_copy(self.own, self.ref, self.recv).start()

    def copy(self, k, device):
        return pltpu.make_async_remote_copy(
            src_ref=self.ref,
            dst_ref=self.ref,
            send_sem=self.send.at[min(k, 1) if len(self.tree.edges) == 2 else k // 2],
            recv_sem=self.recv,
            device_id=device,
            device_id_type=MESH,
        )

    def forward(self):
        def wait():
            pltpu.make_async_copy(self.ref, self.ref, self.recv).wait()

        if self.when is None:
            wait()
        else:
            pl.when(self.when)(wait)
        for k, (cond, device) in enumerate(self.tree.edges):
            @pl.when(self.both(cond))
            def _(k=k, device=device):
                self.copy(k, device).start()

    def finish(self):
        for k, (cond, device) in enumerate(self.tree.edges):
            @pl.when(self.both(cond))
            def _(k=k, device=device):
                self.copy(k, device).wait_send()


def greet_all(n_row, n_col, r, c):
    barrier = pltpu.get_barrier_semaphore()
    for d in range(1, n_row):
        pl.semaphore_signal(barrier, inc=1, device_id=((r + d) % n_row, c), device_id_type=MESH)
    for d in range(1, n_col):
        pl.semaphore_signal(barrier, inc=1, device_id=(r, (c + d) % n_col), device_id_type=MESH)
    pl.semaphore_wait(barrier, n_row + n_col - 2)


def halves(ref_of):
    return ref_of


def spread_kernel(n_row, n_col, panel, pieces_of, *refs):
    r, c = lax.axis_index("row"), lax.axis_index("col")
    send, recv = refs[-2], refs[-1]
    greet_all(n_row, n_col, r, c)
    pieces_of(n_row, n_col, r, c, refs[:-2], send, recv)


def parts(ref, lead, half):
    view = ref if lead is None else ref.at[lead]
    rows = view.shape[0] // 2
    return view.at[pl.ds(half * rows, rows)]


def first_spread(n_row, n_col, r, c, refs, send, recv):
    u, v, up_u, up_v, low_u, low_v, p_u, p_v, q = refs
    rt = row_tree(n_row, 0, r, c)
    ct = col_tree(n_col, 0, r, c)
    qt = col_tree(n_col, 1, r, c)
    count = [0]

    def piece(tree, own, ref, when=None):
        k = count[0]
        count[0] += 1
        return Piece(tree, own, ref, send.at[k], recv.at[k], when)

    first_row = r == 1
    low = [piece(ct, parts(a, 0, h), parts(b, None, h)) for h in range(2) for a, b in ((u, low_u), (v, low_v))]
    chain = [
        piece(rt, parts(a, t, h), parts(b, t, h))
        for t in range(2)
        for a, b in ((u, up_u), (v, up_v))
        for h in range(2)
    ]
    pivot = [
        piece(ct, parts(a, 0, h), parts(b, None, h)) for a, b in ((up_u, p_u), (up_v, p_v)) for h in range(2)
    ]
    q_own = [piece(qt, parts(a, 0, h), parts(q, k, h), first_row) for k, a in ((0, u), (1, v)) for h in range(2)]
    q_up = [
        piece(qt, parts(a, 0, h), parts(q, k, h), first_row) for k, a in ((2, up_u), (3, up_v)) for h in range(2)
    ]
    for x in chain + low + q_own:
        x.begin()
    for x in low:
        x.forward()
    for k in range(4):
        chain[k].forward()
        pivot[k].begin()
        q_up[k].begin()
    for k in range(4):
        chain[4 + k].forward()
        pivot[k].forward()
    for x in q_own + q_up:
        x.forward()
    for x in low + chain + pivot + q_own + q_up:
        x.finish()


def second_spread(n_row, n_col, r, c, refs, send, recv):
    u, v, y, wide, up_y, up_v, low_u, low_v, up_wide = refs
    rt = row_tree(n_row, 1, r, c)
    ct = col_tree(n_col, 1, r, c)
    count = [0]

    def piece(tree, own, ref, when=None):
        k = count[0]
        count[0] += 1
        return Piece(tree, own, ref, send.at[k], recv.at[k], when)

    low = [piece(ct, parts(a, 0, h), parts(b, None, h)) for h in range(2) for a, b in ((u, low_u), (v, low_v))]
    chain = [
        piece(rt, parts(a, t, h), parts(b, t, h))
        for a, b in ((y, up_y), (v, up_v))
        for t in range(2)
        for h in range(2)
    ]
    extra = [piece(rt, parts(wide, None, h), parts(up_wide, None, h), c == 1) for h in range(2)]
    for x in chain + low + extra:
        x.begin()
    for x in low[:2] + chain[:2] + low[2:] + chain[2:] + extra:
        x.forward()
    for x in low + chain + extra:
        x.finish()


def spread(mesh_shape, body, pieces, collective_id, inputs, out_shapes):
    n_row, n_col = mesh_shape
    return pl.pallas_call(
        functools.partial(spread_kernel, n_row, n_col, 0, body),
        out_shape=[jax.ShapeDtypeStruct(s, F32) for s in out_shapes],
        in_specs=[VMEM_SPEC] * len(inputs),
        out_specs=[VMEM_SPEC] * len(out_shapes),
        scratch_shapes=[pltpu.SemaphoreType.DMA((pieces, 2)), pltpu.SemaphoreType.DMA((pieces,))],
        compiler_params=pltpu.CompilerParams(collective_id=collective_id, has_side_effects=True),
    )(*inputs)


def first_panel(n_row, n_col, order, ranks, u, v, up_u, up_v, low_u, low_v, p_u, p_v, q, near, sketch, ou, ov, oy, ow):
    r, c = lax.axis_index("row"), lax.axis_index("col")
    far = 1.0 / (8.0 * u.shape[1])
    pivot_t = near[0].T + far * dot_nt(p_v[...], p_u[...])
    lower = apply_inverse(pivot_t, diagonal_inverse(near[0]), low_v[...])
    lower_t = split(lower.T)
    lead = split(low_u[...])
    wide_of = lambda up: dot_pairs(lead, split(far * dot_pairs(lower_t, split(up))))
    us, vs = [u[t] for t in range(2)], [v[t] for t in range(2)]
    ups = [up_v[t] for t in range(2)]
    wides = [wide_of(up_u[t]) for t in range(2)]
    fresh = recompress(us, vs, wides, ups, sketch[0], [ranks[1, t] for t in range(2)], order)
    for t in range(2):
        j = t * n_col + c
        chosen = (r > 0) & (j > 0) & jnp.logical_not((r == 1) & (j == 1))
        pivot_here = (r == 0) & (j == 0)
        lower_here = (r > 0) & (j == 0)
        ou[t] = jnp.where(pivot_here, 0.0, jnp.where(chosen, fresh[t][0], us[t]))
        ov[t] = jnp.where(pivot_here, 0.0, jnp.where(lower_here, lower, jnp.where(chosen, fresh[t][1], vs[t])))

    @pl.when(r == 1)
    def _():
        wide = wide_of(q[2])
        pivot = near[1] + far * (dot_nt(q[0], q[1]) - dot_nt(wide, q[3]))
        scale = diagonal_inverse(near[1])
        width = u.shape[2]
        y = apply_inverse(pivot, scale, jnp.concatenate([ou[0], ou[1]], axis=1))
        oy[0] = jnp.where(c == 1, q[0], y[:, :width])
        oy[1] = y[:, width:]
        ow[...] = wide


def second_panel(n_row, n_col, order, ranks, u, v, up_y, up_v, low_u, low_v, up_wide, old_v, near, sketch, ou, ov):
    r, c = lax.axis_index("row"), lax.axis_index("col")
    far = 1.0 / (8.0 * u.shape[1])
    lower_t = split(low_v[...].T)
    lead = split(low_u[...])
    us, vs = [u[t] for t in range(2)], [v[t] for t in range(2)]
    ups = [up_v[t] for t in range(2)]
    wides = [dot_pairs(lead, split(far * dot_pairs(lower_t, split(up_y[t])))) for t in range(2)]
    fresh = recompress(us, vs, wides, ups, sketch[1], [ranks[2, t] for t in range(2)], order)
    for t in range(2):
        j = t * n_col + c
        chosen = (r > 1) & (j > 1)
        pivot_here = (r == 1) & (j == 1)
        ou[t] = jnp.where(pivot_here, 0.0, jnp.where(chosen, fresh[t][0], us[t]))
        ov[t] = jnp.where(pivot_here, 0.0, jnp.where(chosen, fresh[t][1], vs[t]))

    @pl.when((c == 1) & (r > 1))
    def _():
        pivot_t = near[1].T + far * (dot_nt(up_v[0], up_y[0]) - dot_nt(old_v[0], up_wide[...]))
        ov[0] = apply_inverse(pivot_t, diagonal_inverse(near[1]), v[0])


def panel_call(body, out_shapes, inputs):
    return pl.pallas_call(
        body,
        out_shape=[jax.ShapeDtypeStruct(s, F32) for s in out_shapes],
        in_specs=[SMEM_SPEC] + [VMEM_SPEC] * (len(inputs) - 1),
        out_specs=[VMEM_SPEC] * len(out_shapes),
        compiler_params=pltpu.CompilerParams(vmem_limit_bytes=60 * 1024 * 1024),
    )(*inputs)


def body(n_row, n_col, factor_u, factor_v, near_field, sketch, tile_ranks):
    tiles, height, width = factor_u.shape[2], factor_u.shape[4], factor_u.shape[5]
    row_here = lax.axis_index("row")
    ranks = lax.dynamic_slice_in_dim(tile_ranks, row_here, 1, 2).reshape(3, tiles)
    keep = (jnp.arange(width, dtype=jnp.int32) < ranks[0][:, None]).astype(F32)[:, None, :]
    u = factor_u.reshape(tiles, height, width) * keep
    v = factor_v.reshape(tiles, height, width) * keep
    pair, one = (tiles, height, width), (height, width)
    shape = (n_row, n_col)
    order_1 = width - max(1, width // 4)
    order_2 = order_1 - max(1, order_1 // 4)
    up_u, up_v, low_u, low_v, p_u, p_v, q = spread(
        shape, first_spread, 24, 0, (u, v), (pair, pair, one, one, one, one, (4, height, width))
    )
    u1, v1, y, wide = panel_call(
        functools.partial(first_panel, n_row, n_col, order_1),
        (pair, pair, pair, one),
        (ranks, u, v, up_u, up_v, low_u, low_v, p_u, p_v, q, near_field, sketch),
    )
    up_y, up_v1, low_u1, low_v1, up_wide = spread(
        shape, second_spread, 14, 1, (u1, v1, y, wide), (pair, pair, one, one, one)
    )
    u2, v2 = panel_call(
        functools.partial(second_panel, n_row, n_col, order_2),
        (pair, pair),
        (ranks, u1, v1, up_y, up_v1, low_u1, low_v1, up_wide, up_v, near_field, sketch),
    )
    shape_out = (1, 1, tiles, 1, height, width)
    return (u2.reshape(shape_out), v2.reshape(shape_out))


def solution(mesh):
    return jax.shard_map(
        functools.partial(body, mesh.shape["row"], mesh.shape["col"]),
        mesh=mesh,
        in_specs=(
            P(None, "row", None, "col", None, None),
            P(None, "row", None, "col", None, None),
            P(),
            P(),
            P(None, None, None, None, "col"),
        ),
        out_specs=(
            P(None, "row", None, "col", None, None),
            P(None, "row", None, "col", None, None),
        ),
        check_vma=False,
    )
```

```python
import functools
import math

import jax
import jax.numpy as jnp
from jax import lax
from jax.experimental import pallas as pl
from jax.experimental.pallas import tpu as pltpu
from jax.sharding import PartitionSpec as P

NS_STEPS = 3
BLOCK = 16
F32 = jnp.float32
BF16 = jnp.bfloat16
VMEM_SPEC = pl.BlockSpec(memory_space=pltpu.VMEM)
SMEM_SPEC = pl.BlockSpec(memory_space=pltpu.SMEM)
MESH = pl.DeviceIdType.MESH


def split(x):
    high = x.astype(BF16)
    return high, (x - high.astype(F32)).astype(BF16)


def dot_pairs(a, b, contract_b=0):
    dims = (((1,), (contract_b,)), ((), ()))
    ah, al = a
    bh, bl = b
    mm = lambda p, q: lax.dot_general(p, q, dims, preferred_element_type=F32)
    return mm(ah, bh) + (mm(ah, bl) + mm(al, bh))


def dot(a, b):
    return dot_pairs(split(a), split(b))


def dot_nt(a, b):
    return dot_pairs(split(a), split(b), 1)


def dot_tn(a, b):
    return dot_pairs(split(a.T), split(b))


def apply_inverse(matrix, scale, w):
    pair = split(matrix)

    def step(level, x):
        if level == 0:
            return scale * x
        y = step(level - 1, x)
        return step(level - 1, 2.0 * x - dot_pairs(pair, split(y)))

    return step(NS_STEPS, w)


def diagonal_inverse(near):
    n = near.shape[0]
    eye = lax.broadcasted_iota(jnp.int32, (n, n), 0) == lax.broadcasted_iota(jnp.int32, (n, n), 1)
    return 1.0 / jnp.sum(jnp.where(eye, near, 0.0), axis=1, keepdims=True)


def cholesky_inverse(grams, order):
    width = grams[0].shape[1]
    count = len(grams)
    eye = (
        lax.broadcasted_iota(jnp.int32, (order, width), 0) == lax.broadcasted_iota(jnp.int32, (order, width), 1)
    ).astype(F32)
    rest = [jnp.concatenate([g[:order], eye], axis=1) for g in grams]
    done = []
    start = 0
    while start < order:
        size = min(BLOCK, order - start)
        row_id = lax.broadcasted_iota(jnp.int32, (1, size, width), 1)
        rows = jnp.stack([x[:size] for x in rest])
        cols = jnp.stack(
            [
                jnp.stack([jnp.broadcast_to(x[:size, start + j : start + j + 1], (size, width)) for x in rest])
                for j in range(size)
            ]
        )
        scale = jnp.ones((count, size, width), F32)
        for k in range(size):
            lead = cols[0]
            inv = lax.rsqrt(lead[:, k : k + 1])
            m = jnp.where(row_id > k, lead * (inv * inv), 0.0)
            if k + 1 < size:
                cols = cols[1:]
                cols = cols - m[None] * cols[:, :, k : k + 1]
            rows = rows - jnp.concatenate([m, m], axis=2) * rows[:, k : k + 1]
            scale = jnp.where(row_id == k, inv, scale)
        rows = rows * jnp.concatenate([scale, scale], axis=2)
        done.append(rows[:, :, width:])
        end = start + size
        if end < order:
            rest = [
                rest[t][size:]
                - jnp.dot(
                    rows[t][:, :width].T[end:order],
                    rows[t],
                    precision=lax.Precision.HIGHEST,
                    preferred_element_type=F32,
                )
                for t in range(count)
            ]
        start = end
    if order < width:
        done.append(jnp.zeros((count, width - order, width), F32))
    inverses = jnp.concatenate(done, axis=1)
    return [inverses[t] for t in range(count)]


def orthonormal(bases, ranks, order):
    width = bases[0].shape[1]
    row = lax.broadcasted_iota(jnp.int32, (width, width), 0)
    col = lax.broadcasted_iota(jnp.int32, (width, width), 1)
    grams = []
    for basis, rank in zip(bases, ranks):
        gram = dot_tn(basis, basis)
        grams.append(gram + jnp.where((row == col) & (col >= rank), 1.0, 0.0))
    inverses = cholesky_inverse(grams, order)
    return [dot_nt(basis, inverse) for basis, inverse in zip(bases, inverses)]


def recompress(us, vs, wides, ups, sketch, ranks, order):
    height, width = us[0].shape
    root_order = math.sqrt(height)
    sk = split(sketch)
    bases = []
    for u, v, wide, up, rank in zip(us, vs, wides, ups, ranks):
        here = dot_pairs(split(v.T), sk)
        above = dot_pairs(split(up.T), sk)
        basis = dot(u, here) - dot(wide, above)
        keep = lax.broadcasted_iota(jnp.int32, (height, width), 1) < rank
        bases.append(jnp.where(keep, basis, 0.0))
    orthos = orthonormal(orthonormal(bases, ranks, order), ranks, order)
    out = []
    for u, v, wide, up, ortho in zip(us, vs, wides, ups, orthos):
        o = split(ortho)
        new_v = dot(v, dot_pairs(split(u.T), o)) - dot(up, dot_pairs(split(wide.T), o))
        out.append((ortho * root_order, new_v * (1.0 / root_order)))
    return out


class Tree:
    def __init__(self, root, edges):
        self.root = root
        self.edges = edges


def row_tree(n, source, r, c):
    levels = n // 2
    level, side, e = r // 2, (r + source) % 2, c % 2
    index = lambda l, s: 2 * l + (s + source) % 2
    spine = side == e
    edges = [
        (spine & (level + 1 < levels), (index(level + 1, e), c)),
        (jnp.logical_not(spine) & (level == 1 - e), (index(0, 1), c)),
        (spine & (level >= 1), (index(level, 1 - e), c)),
    ]
    return Tree((level == 0) & (side == 0), edges)


def col_tree(n, source, r, c):
    levels = n // 2
    level, side = c // 2, (c + source) % 2
    index = lambda l, s: 2 * l + (s + source) % 2
    edges = [
        ((side == 0) & (level + 1 < levels), (r, index(level + 1, 0))),
        (side == 0, (r, index(level, 1))),
    ]
    return Tree((level == 0) & (side == 0), edges)


class Piece:
    def __init__(self, tree, own, ref, send, recv, when=None):
        self.tree, self.own, self.ref, self.send, self.recv, self.when = tree, own, ref, send, recv, when

    def both(self, cond):
        return cond if self.when is None else cond & self.when

    def begin(self):
        @pl.when(self.both(self.tree.root))
        def _():
            pltpu.make_async_copy(self.own, self.ref, self.recv).start()

    def copy(self, k, device):
        return pltpu.make_async_remote_copy(
            src_ref=self.ref,
            dst_ref=self.ref,
            send_sem=self.send.at[min(k, 1) if len(self.tree.edges) == 2 else k // 2],
            recv_sem=self.recv,
            device_id=device,
            device_id_type=MESH,
        )

    def forward(self, only=None):
        both = lambda cond: self.both(cond if only is None else cond & only)

        def wait():
            pltpu.make_async_copy(self.ref, self.ref, self.recv).wait()

        if self.when is None and only is None:
            wait()
        else:
            pl.when(self.when if only is None else self.both(only))(wait)
        for k, (cond, device) in enumerate(self.tree.edges):
            @pl.when(both(cond))
            def _(k=k, device=device):
                self.copy(k, device).start()

    def finish(self):
        for k, (cond, device) in enumerate(self.tree.edges):
            @pl.when(self.both(cond))
            def _(k=k, device=device):
                self.copy(k, device).wait_send()


def greet_all(n_row, n_col, r, c):
    barrier = pltpu.get_barrier_semaphore()
    for d in range(1, n_row):
        pl.semaphore_signal(barrier, inc=1, device_id=((r + d) % n_row, c), device_id_type=MESH)
    for d in range(1, n_col):
        pl.semaphore_signal(barrier, inc=1, device_id=(r, (c + d) % n_col), device_id_type=MESH)
    pl.semaphore_wait(barrier, n_row + n_col - 2)


def parts(ref, lead, half):
    view = ref if lead is None else ref.at[lead]
    rows = view.shape[0] // 2
    return view.at[pl.ds(half * rows, rows)]


def kernel(n_row, n_col, order_1, order_2, ranks, u, v, near, sketch, out_u, out_v, *scratch):
    (up_u, up_v, low_u, low_v, p_u, p_v, q, u1, v1, y, wide_own, up_y, up_v1, low_u1, low_v1, up_wide, send, recv) = scratch
    r, c = lax.axis_index("row"), lax.axis_index("col")
    far = 1.0 / (8.0 * u.shape[1])
    width = u.shape[2]
    greet_all(n_row, n_col, r, c)
    rt0, rt1 = row_tree(n_row, 0, r, c), row_tree(n_row, 1, r, c)
    ct0, ct1 = col_tree(n_col, 0, r, c), col_tree(n_col, 1, r, c)
    pieces = []

    def piece(tree, own, ref, when=None):
        k = len(pieces)
        pieces.append(Piece(tree, own, ref, send.at[k], recv.at[k], when))
        return pieces[-1]

    two = range(2)
    first_row = r == 1
    low = [piece(ct0, parts(a, 0, h), parts(b, None, h)) for h in two for a, b in ((u, low_u), (v, low_v))]
    chain = [piece(rt0, parts(a, t, h), parts(b, t, h)) for t in two for a, b in ((u, up_u), (v, up_v)) for h in two]
    pivot = [piece(ct0, parts(a, 0, h), parts(b, None, h)) for a, b in ((up_u, p_u), (up_v, p_v)) for h in two]
    q_own = [piece(ct1, parts(a, 0, h), parts(q, k, h), first_row) for k, a in ((0, u), (1, v)) for h in two]
    q_up = [piece(ct1, parts(a, 0, h), parts(q, k, h), first_row) for k, a in ((2, up_u), (3, up_v)) for h in two]
    low1 = [piece(ct1, parts(a, 0, h), parts(b, None, h)) for h in two for a, b in ((u1, low_u1), (v1, low_v1))]
    chain_v = [piece(rt1, parts(v1, t, h), parts(up_v1, t, h)) for t in two for h in two]
    chain_y = [piece(rt1, parts(y, t, h), parts(up_y, t, h)) for t in two for h in two]
    extra = [piece(rt1, parts(wide_own, None, h), parts(up_wide, None, h), c == 1) for h in two]

    for x in chain + low + q_own:
        x.begin()
    for x in low:
        x.forward()
    for k in range(4):
        chain[k].forward()
        pivot[k].begin()
        q_up[k].begin()
    for k in range(4):
        chain[4 + k].forward()
        pivot[k].forward()
    for x in q_own + q_up:
        x.forward(c == 1)
    pivot_t = near[0].T + far * dot_nt(p_v[...], p_u[...])
    lower = apply_inverse(pivot_t, diagonal_inverse(near[0]), low_v[...])
    for x in q_own + q_up:
        x.forward(c != 1)
    lower_t = split(lower.T)
    lead = split(low_u[...])
    wide_of = lambda up: dot_pairs(lead, split(far * dot_pairs(lower_t, split(up))))
    us, vs = [u[t] for t in two], [v[t] for t in two]
    fresh = recompress(
        us, vs, [wide_of(up_u[t]) for t in two], [up_v[t] for t in two], sketch[0], [ranks[1, t] for t in two], order_1
    )
    for t in two:
        j = t * n_col + c
        chosen = (r > 0) & (j > 0) & jnp.logical_not((r == 1) & (j == 1))
        pivot_here = (r == 0) & (j == 0)
        lower_here = (r > 0) & (j == 0)
        u1[t] = jnp.where(pivot_here, 0.0, jnp.where(chosen, fresh[t][0], us[t]))
        v1[t] = jnp.where(pivot_here, 0.0, jnp.where(lower_here, lower, jnp.where(chosen, fresh[t][1], vs[t])))

    @pl.when(first_row)
    def _():
        wide_own[...] = wide_of(q[2])

    for x in low1 + chain_v + extra:
        x.begin()
    for x in low1 + chain_v + extra:
        x.forward()

    @pl.when(first_row)
    def _():
        pivot_1 = near[1] + far * (dot_nt(q[0], q[1]) - dot_nt(wide_own[...], q[3]))
        applied = apply_inverse(pivot_1, diagonal_inverse(near[1]), jnp.concatenate([u1[0], u1[1]], axis=1))
        y[0] = jnp.where(c == 1, q[0], applied[:, :width])
        y[1] = applied[:, width:]

    for x in chain_y:
        x.begin()
    for x in chain_y:
        x.forward()
    lower_t1 = split(low_v1[...].T)
    lead_1 = split(low_u1[...])
    us, vs = [u1[t] for t in two], [v1[t] for t in two]
    wides = [dot_pairs(lead_1, split(far * dot_pairs(lower_t1, split(up_y[t])))) for t in two]
    fresh = recompress(us, vs, wides, [up_v1[t] for t in two], sketch[1], [ranks[2, t] for t in two], order_2)
    for t in two:
        j = t * n_col + c
        chosen = (r > 1) & (j > 1)
        pivot_here = (r == 1) & (j == 1)
        out_u[t] = jnp.where(pivot_here, 0.0, jnp.where(chosen, fresh[t][0], us[t]))
        out_v[t] = jnp.where(pivot_here, 0.0, jnp.where(chosen, fresh[t][1], vs[t]))

    @pl.when((c == 1) & (r > 1))
    def _():
        pivot_1t = near[1].T + far * (dot_nt(up_v1[0], up_y[0]) - dot_nt(up_v[0], up_wide[...]))
        out_v[0] = apply_inverse(pivot_1t, diagonal_inverse(near[1]), v1[0])

    for x in pieces:
        x.finish()


def body(n_row, n_col, factor_u, factor_v, near_field, sketch, tile_ranks):
    tiles, height, width = factor_u.shape[2], factor_u.shape[4], factor_u.shape[5]
    row_here = lax.axis_index("row")
    ranks = lax.dynamic_slice_in_dim(tile_ranks, row_here, 1, 2).reshape(3, tiles)
    keep = (jnp.arange(width, dtype=jnp.int32) < ranks[0][:, None]).astype(F32)[:, None, :]
    u = factor_u.reshape(tiles, height, width) * keep
    v = factor_v.reshape(tiles, height, width) * keep
    pair, one = (tiles, height, width), (height, width)
    order_1 = width - max(1, width // 4)
    order_2 = order_1 - max(1, order_1 // 4)
    buffers = [pair, pair, one, one, one, one, (4, height, width), pair, pair, pair, one, pair, pair, one, one, one]
    pieces = 38
    out_u, out_v = pl.pallas_call(
        functools.partial(kernel, n_row, n_col, order_1, order_2),
        out_shape=[jax.ShapeDtypeStruct(pair, F32)] * 2,
        in_specs=[SMEM_SPEC] + [VMEM_SPEC] * 4,
        out_specs=[VMEM_SPEC] * 2,
        scratch_shapes=[pltpu.VMEM(s, F32) for s in buffers]
        + [pltpu.SemaphoreType.DMA((pieces, 2)), pltpu.SemaphoreType.DMA((pieces,))],
        compiler_params=pltpu.CompilerParams(
            collective_id=0, has_side_effects=True, vmem_limit_bytes=60 * 1024 * 1024
        ),
    )(ranks, u, v, near_field, sketch)
    shape_out = (1, 1, tiles, 1, height, width)
    return (out_u.reshape(shape_out), out_v.reshape(shape_out))


def solution(mesh):
    return jax.shard_map(
        functools.partial(body, mesh.shape["row"], mesh.shape["col"]),
        mesh=mesh,
        in_specs=(
            P(None, "row", None, "col", None, None),
            P(None, "row", None, "col", None, None),
            P(),
            P(),
            P(None, None, None, None, "col"),
        ),
        out_specs=(
            P(None, "row", None, "col", None, None),
            P(None, "row", None, "col", None, None),
        ),
        check_vma=False,
    )
```

```python
import functools
import math

import jax
import jax.numpy as jnp
from jax import lax
from jax.experimental import pallas as pl
from jax.experimental.pallas import tpu as pltpu
from jax.sharding import PartitionSpec as P

NS_STEPS = 3
BLOCK = 16
F32 = jnp.float32
BF16 = jnp.bfloat16
VMEM_SPEC = pl.BlockSpec(memory_space=pltpu.VMEM)
SMEM_SPEC = pl.BlockSpec(memory_space=pltpu.SMEM)
MESH = pl.DeviceIdType.MESH


def split(x):
    high = x.astype(BF16)
    return high, (x - high.astype(F32)).astype(BF16)


def dot_pairs(a, b, contract_b=0):
    dims = (((1,), (contract_b,)), ((), ()))
    ah, al = a
    bh, bl = b
    mm = lambda p, q: lax.dot_general(p, q, dims, preferred_element_type=F32)
    return mm(ah, bh) + (mm(ah, bl) + mm(al, bh))


def dot(a, b):
    return dot_pairs(split(a), split(b))


def dot_nt(a, b):
    return dot_pairs(split(a), split(b), 1)


def dot_tn(a, b):
    return dot_pairs(split(a.T), split(b))


def apply_inverse(matrix, scale, w):
    pair = split(matrix)

    def step(level, x):
        if level == 0:
            return scale * x
        y = step(level - 1, x)
        return step(level - 1, 2.0 * x - dot_pairs(pair, split(y)))

    return step(NS_STEPS, w)


def diagonal_inverse(near):
    n = near.shape[0]
    eye = lax.broadcasted_iota(jnp.int32, (n, n), 0) == lax.broadcasted_iota(jnp.int32, (n, n), 1)
    return 1.0 / jnp.sum(jnp.where(eye, near, 0.0), axis=1, keepdims=True)


def cholesky_inverse(grams, order):
    width = grams[0].shape[1]
    count = len(grams)
    eye = (
        lax.broadcasted_iota(jnp.int32, (order, width), 0) == lax.broadcasted_iota(jnp.int32, (order, width), 1)
    ).astype(F32)
    rest = [jnp.concatenate([g[:order], eye], axis=1) for g in grams]
    done = []
    start = 0
    while start < order:
        size = min(BLOCK, order - start)
        row_id = lax.broadcasted_iota(jnp.int32, (1, size, width), 1)
        rows = jnp.stack([x[:size] for x in rest])
        cols = jnp.stack(
            [
                jnp.stack([jnp.broadcast_to(x[:size, start + j : start + j + 1], (size, width)) for x in rest])
                for j in range(size)
            ]
        )
        scale = jnp.ones((count, size, width), F32)
        for k in range(size):
            lead = cols[0]
            inv = lax.rsqrt(lead[:, k : k + 1])
            m = jnp.where(row_id > k, lead * (inv * inv), 0.0)
            if k + 1 < size:
                cols = cols[1:]
                cols = cols - m[None] * cols[:, :, k : k + 1]
            rows = rows - jnp.concatenate([m, m], axis=2) * rows[:, k : k + 1]
            scale = jnp.where(row_id == k, inv, scale)
        rows = rows * jnp.concatenate([scale, scale], axis=2)
        done.append(rows[:, :, width:])
        end = start + size
        if end < order:
            rest = [
                rest[t][size:]
                - jnp.dot(
                    rows[t][:, :width].T[end:order],
                    rows[t],
                    precision=lax.Precision.HIGHEST,
                    preferred_element_type=F32,
                )
                for t in range(count)
            ]
        start = end
    if order < width:
        done.append(jnp.zeros((count, width - order, width), F32))
    inverses = jnp.concatenate(done, axis=1)
    return [inverses[t] for t in range(count)]


def orthonormal(bases, ranks, order):
    width = bases[0].shape[1]
    row = lax.broadcasted_iota(jnp.int32, (width, width), 0)
    col = lax.broadcasted_iota(jnp.int32, (width, width), 1)
    grams = []
    for basis, rank in zip(bases, ranks):
        gram = dot_tn(basis, basis)
        grams.append(gram + jnp.where((row == col) & (col >= rank), 1.0, 0.0))
    inverses = cholesky_inverse(grams, order)
    return [dot_nt(basis, inverse) for basis, inverse in zip(bases, inverses)]


def recompress(us, vs, wides, ups, sketch, ranks, order):
    height, width = us[0].shape
    root_order = math.sqrt(height)
    sk = split(sketch)
    bases = []
    for u, v, wide, up, rank in zip(us, vs, wides, ups, ranks):
        here = dot_pairs(split(v.T), sk)
        above = dot_pairs(split(up.T), sk)
        basis = dot(u, here) - dot(wide, above)
        keep = lax.broadcasted_iota(jnp.int32, (height, width), 1) < rank
        bases.append(jnp.where(keep, basis, 0.0))
    orthos = orthonormal(orthonormal(bases, ranks, order), ranks, order)
    out = []
    for u, v, wide, up, ortho in zip(us, vs, wides, ups, orthos):
        o = split(ortho)
        new_v = dot(v, dot_pairs(split(u.T), o)) - dot(up, dot_pairs(split(wide.T), o))
        out.append((ortho * root_order, new_v * (1.0 / root_order)))
    return out


class Tree:
    def __init__(self, root, edges):
        self.root = root
        self.edges = edges


def row_tree(n, source, r, c, direct=False):
    levels = n // 2
    level, side, e = r // 2, (r + source) % 2, c % 2
    index = lambda l, s: 2 * l + (s + source) % 2
    spine = side == e
    edges = [
        (spine & (level + 1 < levels), (index(level + 1, e), c)),
        ((level == 0) & (side == 0) if direct else jnp.logical_not(spine) & (level == 1 - e), (index(0, 1), c)),
        (spine & (level >= 1), (index(level, 1 - e), c)),
    ]
    return Tree((level == 0) & (side == 0), edges)


def col_tree(n, source, r, c):
    levels = n // 2
    level, side = c // 2, (c + source) % 2
    index = lambda l, s: 2 * l + (s + source) % 2
    edges = [
        ((side == 0) & (level + 1 < levels), (r, index(level + 1, 0))),
        (side == 0, (r, index(level, 1))),
    ]
    return Tree((level == 0) & (side == 0), edges)


class Piece:
    def __init__(self, tree, own, ref, send, recv, when=None):
        self.tree, self.own, self.ref, self.send, self.recv, self.when = tree, own, ref, send, recv, when

    def both(self, cond):
        return cond if self.when is None else cond & self.when

    def begin(self):
        @pl.when(self.both(self.tree.root))
        def _():
            pltpu.make_async_copy(self.own, self.ref, self.recv).start()

    def copy(self, k, device):
        return pltpu.make_async_remote_copy(
            src_ref=self.ref,
            dst_ref=self.ref,
            send_sem=self.send.at[min(k, 1)],
            recv_sem=self.recv,
            device_id=device,
            device_id_type=MESH,
        )

    def forward(self, only=None):
        both = lambda cond: self.both(cond if only is None else cond & only)

        def wait():
            pltpu.make_async_copy(self.ref, self.ref, self.recv).wait()

        if self.when is None and only is None:
            wait()
        else:
            pl.when(self.when if only is None else self.both(only))(wait)
        for k, (cond, device) in enumerate(self.tree.edges):
            @pl.when(both(cond))
            def _(k=k, device=device):
                self.copy(k, device).start()

    def finish(self):
        for k, (cond, device) in enumerate(self.tree.edges):
            @pl.when(self.both(cond))
            def _(k=k, device=device):
                self.copy(k, device).wait_send()


def greet_all(n_row, n_col, r, c):
    barrier = pltpu.get_barrier_semaphore()
    for d in range(1, n_row):
        pl.semaphore_signal(barrier, inc=1, device_id=((r + d) % n_row, c), device_id_type=MESH)
    for d in range(1, n_col):
        pl.semaphore_signal(barrier, inc=1, device_id=(r, (c + d) % n_col), device_id_type=MESH)
    pl.semaphore_wait(barrier, n_row + n_col - 2)


def parts(ref, lead, part, count=2):
    view = ref if lead is None else ref.at[lead]
    rows = view.shape[0] // count
    return view.at[pl.ds(part * rows, rows)]


def kernel(n_row, n_col, order_1, order_2, ranks, u, v, near, sketch, out_u, out_v, *scratch):
    (up_u, up_v, low_u, low_v, p_u, p_v, q, u1, v1, y, wide_own, up_y, up_v1, low_u1, low_v1, up_pivot, lower_1, send, recv) = scratch
    r, c = lax.axis_index("row"), lax.axis_index("col")
    far = 1.0 / (8.0 * u.shape[1])
    width = u.shape[2]
    greet_all(n_row, n_col, r, c)
    rt0, rt1 = row_tree(n_row, 0, r, c), row_tree(n_row, 1, r, c)
    rt0_first = row_tree(n_row, 0, r, c, True)
    ct0, ct1 = col_tree(n_col, 0, r, c), col_tree(n_col, 1, r, c)
    pieces = []

    def piece(tree, own, ref, when=None):
        k = len(pieces)
        pieces.append(Piece(tree, own, ref, send.at[k], recv.at[k], when))
        return pieces[-1]

    two = range(2)
    first_row = r == 1
    low = [piece(ct0, parts(a, 0, h), parts(b, None, h)) for h in two for a, b in ((u, low_u), (v, low_v))]
    chain = [
        piece(tree, parts(a, t, h), parts(b, t, h))
        for t, tree in ((0, rt0_first), (1, rt0))
        for a, b in ((u, up_u), (v, up_v))
        for h in two
    ]
    pivot = [piece(ct0, parts(a, 0, h), parts(b, None, h)) for a, b in ((up_u, p_u), (up_v, p_v)) for h in two]
    q_own = [piece(ct1, parts(a, 0, h), parts(q, k, h), first_row) for k, a in ((0, u), (1, v)) for h in two]
    q_up = [piece(ct1, parts(a, 0, h), parts(q, k, h), first_row) for k, a in ((2, up_u), (3, up_v)) for h in two]
    low1 = [piece(ct1, parts(a, 0, h), parts(b, None, h)) for h in two for a, b in ((u1, low_u1), (v1, low_v1))]
    chain_v = [
        piece(rt1, parts(v1, t, h), parts(up_v1, t, h), when) for t, when in ((0, c != 1), (1, None)) for h in two
    ]
    quarters = range(4)
    chain_y = [
        piece(rt1, parts(y, t, h, 4), parts(up_y, t, h, 4), when)
        for t, when in ((0, c != 1), (1, None))
        for h in quarters
    ]
    extra = [
        piece(rt1, parts(a, lead, h), parts(up_pivot, k, h), c == 1)
        for k, a, lead in ((0, wide_own, None), (1, u1, 0), (2, v1, 0))
        for h in two
    ]

    for x in chain + low + q_own:
        x.begin()
    for x in low:
        x.forward()
    for k in range(4):
        chain[k].forward()
        pivot[k].begin()
        q_up[k].begin()
    for k in range(4):
        chain[4 + k].forward()
        pivot[k].forward()
    for x in q_own + q_up:
        x.forward(c == 1)
    pivot_t = near[0].T + far * dot_nt(p_v[...], p_u[...])
    lower = apply_inverse(pivot_t, diagonal_inverse(near[0]), low_v[...])
    for x in q_own + q_up:
        x.forward(c != 1)
    lower_t = split(lower.T)
    lead = split(low_u[...])
    wide_of = lambda up: dot_pairs(lead, split(far * dot_pairs(lower_t, split(up))))
    us, vs = [u[t] for t in two], [v[t] for t in two]
    fresh = recompress(
        us, vs, [wide_of(up_u[t]) for t in two], [up_v[t] for t in two], sketch[0], [ranks[1, t] for t in two], order_1
    )
    for t in two:
        j = t * n_col + c
        chosen = (r > 0) & (j > 0) & jnp.logical_not((r == 1) & (j == 1))
        pivot_here = (r == 0) & (j == 0)
        lower_here = (r > 0) & (j == 0)
        u1[t] = jnp.where(pivot_here, 0.0, jnp.where(chosen, fresh[t][0], us[t]))
        v1[t] = jnp.where(pivot_here, 0.0, jnp.where(lower_here, lower, jnp.where(chosen, fresh[t][1], vs[t])))

    @pl.when(first_row)
    def _():
        wide_own[...] = wide_of(q[2])

    for x in low1 + extra + chain_v:
        x.begin()
    for x in low1 + extra:
        x.forward()
    for x in chain_v:
        x.forward(first_row)

    @pl.when((c == 1) & (r > 1))
    def _():
        pivot_1t = near[1].T + far * (dot_nt(up_pivot[2], up_pivot[1]) - dot_nt(up_v[0], up_pivot[0]))
        lower_1[...] = apply_inverse(pivot_1t, diagonal_inverse(near[1]), v1[0])

    for x in chain_v:
        x.forward(r != 1)

    @pl.when(first_row)
    def _():
        pivot_1 = near[1] + far * (dot_nt(q[0], q[1]) - dot_nt(wide_own[...], q[3]))
        applied = apply_inverse(pivot_1, diagonal_inverse(near[1]), jnp.concatenate([u1[0], u1[1]], axis=1))
        y[0] = applied[:, :width]
        y[1] = applied[:, width:]

    for x in chain_y:
        x.begin()
    for x in chain_y:
        x.forward()
    lower_t1 = split(low_v1[...].T)
    lead_1 = split(low_u1[...])
    us, vs = [u1[t] for t in two], [v1[t] for t in two]
    wides = [dot_pairs(lead_1, split(far * dot_pairs(lower_t1, split(up_y[t])))) for t in two]
    fresh = recompress(us, vs, wides, [up_v1[t] for t in two], sketch[1], [ranks[2, t] for t in two], order_2)
    for t in two:
        j = t * n_col + c
        chosen = (r > 1) & (j > 1)
        out_u[t] = jnp.where(chosen, fresh[t][0], us[t])
        out_v[t] = jnp.where(chosen, fresh[t][1], vs[t])

    @pl.when((c == 1) & (r > 1))
    def _():
        out_v[0] = lower_1[...]

    for x in pieces:
        x.finish()


def body(n_row, n_col, factor_u, factor_v, near_field, sketch, tile_ranks):
    tiles, height, width = factor_u.shape[2], factor_u.shape[4], factor_u.shape[5]
    row_here = lax.axis_index("row")
    ranks = lax.dynamic_slice_in_dim(tile_ranks, row_here, 1, 2).reshape(3, tiles)
    keep = (jnp.arange(width, dtype=jnp.int32) < ranks[0][:, None]).astype(F32)[:, None, :]
    u = factor_u.reshape(tiles, height, width) * keep
    v = factor_v.reshape(tiles, height, width) * keep
    pair, one = (tiles, height, width), (height, width)
    order_1 = width - max(1, width // 4)
    order_2 = order_1 - max(1, order_1 // 4)
    buffers = [pair, pair, one, one, one, one, (4, height, width), pair, pair, pair, one, pair, pair, one, one, (3, height, width), one]
    pieces = 46
    out_u, out_v = pl.pallas_call(
        functools.partial(kernel, n_row, n_col, order_1, order_2),
        out_shape=[jax.ShapeDtypeStruct(pair, F32)] * 2,
        in_specs=[SMEM_SPEC] + [VMEM_SPEC] * 4,
        out_specs=[VMEM_SPEC] * 2,
        scratch_shapes=[pltpu.VMEM(s, F32) for s in buffers]
        + [pltpu.SemaphoreType.DMA((pieces, 2)), pltpu.SemaphoreType.DMA((pieces,))],
        compiler_params=pltpu.CompilerParams(
            collective_id=0, has_side_effects=True, vmem_limit_bytes=60 * 1024 * 1024
        ),
    )(ranks, u, v, near_field, sketch)
    tile_col = jnp.arange(tiles, dtype=jnp.int32) * n_col + lax.axis_index("col")
    stays = jnp.logical_not((row_here == 1) & (tile_col == 1))[:, None, None]
    out_u, out_v = jnp.where(stays, out_u, 0.0), jnp.where(stays, out_v, 0.0)
    shape_out = (1, 1, tiles, 1, height, width)
    return (out_u.reshape(shape_out), out_v.reshape(shape_out))


def solution(mesh):
    return jax.shard_map(
        functools.partial(body, mesh.shape["row"], mesh.shape["col"]),
        mesh=mesh,
        in_specs=(
            P(None, "row", None, "col", None, None),
            P(None, "row", None, "col", None, None),
            P(),
            P(),
            P(None, None, None, None, "col"),
        ),
        out_specs=(
            P(None, "row", None, "col", None, None),
            P(None, "row", None, "col", None, None),
        ),
        check_vma=False,
    )
```

```python
import functools
import math

import jax
import jax.numpy as jnp
from jax import lax
from jax.experimental import pallas as pl
from jax.experimental.pallas import tpu as pltpu
from jax.sharding import PartitionSpec as P

NS_STEPS = 3
BLOCK = 16
F32 = jnp.float32
BF16 = jnp.bfloat16
VMEM_SPEC = pl.BlockSpec(memory_space=pltpu.VMEM)
SMEM_SPEC = pl.BlockSpec(memory_space=pltpu.SMEM)
MESH = pl.DeviceIdType.MESH


def split(x):
    high = x.astype(BF16)
    return high, (x - high.astype(F32)).astype(BF16)


def dot_pairs(a, b, contract_b=0):
    dims = (((1,), (contract_b,)), ((), ()))
    ah, al = a
    bh, bl = b
    mm = lambda p, q: lax.dot_general(p, q, dims, preferred_element_type=F32)
    return mm(ah, bh) + (mm(ah, bl) + mm(al, bh))


def dot(a, b):
    return dot_pairs(split(a), split(b))


def dot_nt(a, b):
    return dot_pairs(split(a), split(b), 1)


def dot_tn(a, b):
    return dot_pairs(split(a.T), split(b))


def apply_inverse(matrix, scale, w):
    pair = split(matrix)

    def step(level, x):
        if level == 0:
            return scale * x
        y = step(level - 1, x)
        return step(level - 1, 2.0 * x - dot_pairs(pair, split(y)))

    return step(NS_STEPS, w)


def diagonal_inverse(near):
    n = near.shape[0]
    eye = lax.broadcasted_iota(jnp.int32, (n, n), 0) == lax.broadcasted_iota(jnp.int32, (n, n), 1)
    return 1.0 / jnp.sum(jnp.where(eye, near, 0.0), axis=1, keepdims=True)


def cholesky_inverse(grams, order):
    width = grams[0].shape[1]
    count = len(grams)
    eye = (
        lax.broadcasted_iota(jnp.int32, (order, width), 0) == lax.broadcasted_iota(jnp.int32, (order, width), 1)
    ).astype(F32)
    rest = [jnp.concatenate([g[:order], eye], axis=1) for g in grams]
    done = []
    start = 0
    while start < order:
        size = min(BLOCK, order - start)
        row_id = lax.broadcasted_iota(jnp.int32, (1, size, width), 1)
        rows = jnp.stack([x[:size] for x in rest])
        cols = jnp.stack(
            [
                jnp.stack([jnp.broadcast_to(x[:size, start + j : start + j + 1], (size, width)) for x in rest])
                for j in range(size)
            ]
        )
        scale = jnp.ones((count, size, width), F32)
        for k in range(size):
            lead = cols[0]
            inv = lax.rsqrt(lead[:, k : k + 1])
            m = jnp.where(row_id > k, lead * (inv * inv), 0.0)
            if k + 1 < size:
                cols = cols[1:]
                cols = cols - m[None] * cols[:, :, k : k + 1]
            rows = rows - jnp.concatenate([m, m], axis=2) * rows[:, k : k + 1]
            scale = jnp.where(row_id == k, inv, scale)
        rows = rows * jnp.concatenate([scale, scale], axis=2)
        done.append(rows[:, :, width:])
        end = start + size
        if end < order:
            rest = [
                rest[t][size:]
                - jnp.dot(
                    rows[t][:, :width].T[end:order],
                    rows[t],
                    precision=lax.Precision.HIGHEST,
                    preferred_element_type=F32,
                )
                for t in range(count)
            ]
        start = end
    if order < width:
        done.append(jnp.zeros((count, width - order, width), F32))
    inverses = jnp.concatenate(done, axis=1)
    return [inverses[t] for t in range(count)]


def orthonormal(bases, ranks, order):
    width = bases[0].shape[1]
    row = lax.broadcasted_iota(jnp.int32, (width, width), 0)
    col = lax.broadcasted_iota(jnp.int32, (width, width), 1)
    grams = []
    for basis, rank in zip(bases, ranks):
        gram = dot_tn(basis, basis)
        grams.append(gram + jnp.where((row == col) & (col >= rank), 1.0, 0.0))
    inverses = cholesky_inverse(grams, order)
    return [dot_nt(basis, inverse) for basis, inverse in zip(bases, inverses)]


def recompress(us, vs, wides, ups, sketch, ranks, order):
    height, width = us[0].shape
    root_order = math.sqrt(height)
    sk = split(sketch)
    bases = []
    for u, v, wide, up, rank in zip(us, vs, wides, ups, ranks):
        here = dot_pairs(split(v.T), sk)
        above = dot_pairs(split(up.T), sk)
        basis = dot(u, here) - dot(wide, above)
        keep = lax.broadcasted_iota(jnp.int32, (height, width), 1) < rank
        bases.append(jnp.where(keep, basis, 0.0))
    orthos = orthonormal(orthonormal(bases, ranks, order), ranks, order)
    out = []
    for u, v, wide, up, ortho in zip(us, vs, wides, ups, orthos):
        o = split(ortho)
        new_v = dot(v, dot_pairs(split(u.T), o)) - dot(up, dot_pairs(split(wide.T), o))
        out.append((ortho * root_order, new_v * (1.0 / root_order)))
    return out


class Tree:
    def __init__(self, root, edges):
        self.root = root
        self.edges = edges


def row_tree(n, source, r, c, direct=False):
    levels = n // 2
    level, side, e = r // 2, (r + source) % 2, c % 2
    index = lambda l, s: 2 * l + (s + source) % 2
    spine = side == e
    edges = [
        (spine & (level + 1 < levels), (index(level + 1, e), c)),
        ((level == 0) & (side == 0) if direct else jnp.logical_not(spine) & (level == 1 - e), (index(0, 1), c)),
        (spine & (level >= 1), (index(level, 1 - e), c)),
    ]
    return Tree((level == 0) & (side == 0), edges)


def col_tree(n, source, r, c):
    levels = n // 2
    level, side = c // 2, (c + source) % 2
    index = lambda l, s: 2 * l + (s + source) % 2
    edges = [
        ((side == 0) & (level + 1 < levels), (r, index(level + 1, 0))),
        (side == 0, (r, index(level, 1))),
    ]
    return Tree((level == 0) & (side == 0), edges)


class Piece:
    def __init__(self, tree, own, ref, send, recv, when=None):
        self.tree, self.own, self.ref, self.send, self.recv, self.when = tree, own, ref, send, recv, when

    def both(self, cond):
        return cond if self.when is None else cond & self.when

    def begin(self):
        @pl.when(self.both(self.tree.root))
        def _():
            pltpu.make_async_copy(self.own, self.ref, self.recv).start()

    def copy(self, k, device):
        return pltpu.make_async_remote_copy(
            src_ref=self.ref,
            dst_ref=self.ref,
            send_sem=self.send.at[min(k, 1)],
            recv_sem=self.recv,
            device_id=device,
            device_id_type=MESH,
        )

    def forward(self, only=None):
        both = lambda cond: self.both(cond if only is None else cond & only)

        def wait():
            pltpu.make_async_copy(self.ref, self.ref, self.recv).wait()

        if self.when is None and only is None:
            wait()
        else:
            pl.when(self.when if only is None else self.both(only))(wait)
        for k, (cond, device) in enumerate(self.tree.edges):
            @pl.when(both(cond))
            def _(k=k, device=device):
                self.copy(k, device).start()

    def finish(self):
        for k, (cond, device) in enumerate(self.tree.edges):
            @pl.when(self.both(cond))
            def _(k=k, device=device):
                self.copy(k, device).wait_send()


def greet_all(n_row, n_col, r, c):
    barrier = pltpu.get_barrier_semaphore()
    for d in range(1, n_row):
        pl.semaphore_signal(barrier, inc=1, device_id=((r + d) % n_row, c), device_id_type=MESH)
    for d in range(1, n_col):
        pl.semaphore_signal(barrier, inc=1, device_id=(r, (c + d) % n_col), device_id_type=MESH)
    pl.semaphore_wait(barrier, n_row + n_col - 2)


def parts(ref, lead, part, count=2):
    view = ref if lead is None else ref.at[lead]
    rows = view.shape[0] // count
    return view.at[pl.ds(part * rows, rows)]


def kernel(n_row, n_col, order_1, order_2, ranks, u, v, near, sketch, out_u, out_v, *scratch):
    (up_u, up_v, low_u, low_v, p_u, p_v, q, u1, v1, y, wide_own, up_y, up_v1, low_u1, low_v1, up_pivot, lower_1, send, recv) = scratch
    r, c = lax.axis_index("row"), lax.axis_index("col")
    far = 1.0 / (8.0 * u.shape[1])
    width = u.shape[2]
    greet_all(n_row, n_col, r, c)
    rt0, rt1 = row_tree(n_row, 0, r, c), row_tree(n_row, 1, r, c)
    rt0_first = row_tree(n_row, 0, r, c, True)
    ct0, ct1 = col_tree(n_col, 0, r, c), col_tree(n_col, 1, r, c)
    pieces = []

    def piece(tree, own, ref, when=None):
        k = len(pieces)
        pieces.append(Piece(tree, own, ref, send.at[k], recv.at[k], when))
        return pieces[-1]

    two = range(2)
    first_row = r == 1
    low = [piece(ct0, parts(a, 0, h), parts(b, None, h)) for h in two for a, b in ((u, low_u), (v, low_v))]
    chain = [
        piece(tree, parts(a, t, h), parts(b, t, h))
        for t, tree in ((0, rt0_first), (1, rt0))
        for a, b in ((u, up_u), (v, up_v))
        for h in two
    ]
    pivot = [piece(ct0, parts(a, 0, h), parts(b, None, h)) for a, b in ((up_u, p_u), (up_v, p_v)) for h in two]
    q_own = [piece(ct1, parts(a, 0, h), parts(q, k, h), first_row) for k, a in ((0, u), (1, v)) for h in two]
    q_up = [piece(ct1, parts(a, 0, h), parts(q, k, h), first_row) for k, a in ((2, up_u), (3, up_v)) for h in two]
    low1 = [piece(ct1, parts(a, 0, h), parts(b, None, h)) for h in two for a, b in ((u1, low_u1), (v1, low_v1))]
    chain_v = [
        piece(rt1, parts(v1, t, h), parts(up_v1, t, h), when) for t, when in ((0, c != 1), (1, None)) for h in two
    ]
    quarters = range(4)
    chain_y = [
        piece(rt1, parts(y, t, h, 4), parts(up_y, t, h, 4), when)
        for t, when in ((0, c != 1), (1, None))
        for h in quarters
    ]
    extra = [
        piece(rt1, parts(a, lead, h), parts(up_pivot, k, h), c == 1)
        for k, a, lead in ((0, wide_own, None), (1, u1, 0), (2, v1, 0))
        for h in two
    ]

    for x in chain + low + q_own:
        x.begin()
    for x in low:
        x.forward()
    for k in range(4):
        chain[k].forward()
        pivot[k].begin()
        q_up[k].begin()
    for k in range(4):
        chain[4 + k].forward()
        pivot[k].forward()
    for x in q_own + q_up:
        x.forward(c == 1)
    pivot_t = near[0].T + far * dot_nt(p_v[...], p_u[...])
    lower = apply_inverse(pivot_t, diagonal_inverse(near[0]), low_v[...])
    lower_t = split(lower.T)
    lead = split(low_u[...])
    wide_of = lambda up: dot_pairs(lead, split(far * dot_pairs(lower_t, split(up))))
    us, vs = [u[t] for t in two], [v[t] for t in two]
    fresh = recompress(
        us, vs, [wide_of(up_u[t]) for t in two], [up_v[t] for t in two], sketch[0], [ranks[1, t] for t in two], order_1
    )
    for t in two:
        j = t * n_col + c
        chosen = (r > 0) & (j > 0) & jnp.logical_not((r == 1) & (j == 1))
        pivot_here = (r == 0) & (j == 0)
        lower_here = (r > 0) & (j == 0)
        u1[t] = jnp.where(pivot_here, 0.0, jnp.where(chosen, fresh[t][0], us[t]))
        v1[t] = jnp.where(pivot_here, 0.0, jnp.where(lower_here, lower, jnp.where(chosen, fresh[t][1], vs[t])))

    for x in q_own + q_up:
        x.forward(c != 1)

    @pl.when(first_row)
    def _():
        wide_own[...] = wide_of(q[2])

    for x in low1 + extra + chain_v:
        x.begin()
    for x in low1 + extra:
        x.forward()
    for x in chain_v:
        x.forward(first_row)

    @pl.when((c == 1) & (r > 1))
    def _():
        pivot_1t = near[1].T + far * (dot_nt(up_pivot[2], up_pivot[1]) - dot_nt(up_v[0], up_pivot[0]))
        lower_1[...] = apply_inverse(pivot_1t, diagonal_inverse(near[1]), v1[0])

    for x in chain_v:
        x.forward(r != 1)

    @pl.when(first_row)
    def _():
        pivot_1 = near[1] + far * (dot_nt(q[0], q[1]) - dot_nt(wide_own[...], q[3]))
        applied = apply_inverse(pivot_1, diagonal_inverse(near[1]), jnp.concatenate([u1[0], u1[1]], axis=1))
        y[0] = applied[:, :width]
        y[1] = applied[:, width:]

    for x in chain_y:
        x.begin()
    for x in chain_y:
        x.forward()
    lower_t1 = split(low_v1[...].T)
    lead_1 = split(low_u1[...])
    us, vs = [u1[t] for t in two], [v1[t] for t in two]
    wides = [dot_pairs(lead_1, split(far * dot_pairs(lower_t1, split(up_y[t])))) for t in two]
    fresh = recompress(us, vs, wides, [up_v1[t] for t in two], sketch[1], [ranks[2, t] for t in two], order_2)
    for t in two:
        j = t * n_col + c
        chosen = (r > 1) & (j > 1)
        out_u[t] = jnp.where(chosen, fresh[t][0], us[t])
        out_v[t] = jnp.where(chosen, fresh[t][1], vs[t])

    @pl.when((c == 1) & (r > 1))
    def _():
        out_v[0] = lower_1[...]

    for x in pieces:
        x.finish()


def body(n_row, n_col, factor_u, factor_v, near_field, sketch, tile_ranks):
    tiles, height, width = factor_u.shape[2], factor_u.shape[4], factor_u.shape[5]
    row_here = lax.axis_index("row")
    ranks = lax.dynamic_slice_in_dim(tile_ranks, row_here, 1, 2).reshape(3, tiles)
    keep = (jnp.arange(width, dtype=jnp.int32) < ranks[0][:, None]).astype(F32)[:, None, :]
    u = factor_u.reshape(tiles, height, width) * keep
    v = factor_v.reshape(tiles, height, width) * keep
    pair, one = (tiles, height, width), (height, width)
    order_1 = width - max(1, width // 4)
    order_2 = order_1 - max(1, order_1 // 4)
    buffers = [pair, pair, one, one, one, one, (4, height, width), pair, pair, pair, one, pair, pair, one, one, (3, height, width), one]
    pieces = 46
    out_u, out_v = pl.pallas_call(
        functools.partial(kernel, n_row, n_col, order_1, order_2),
        out_shape=[jax.ShapeDtypeStruct(pair, F32)] * 2,
        in_specs=[SMEM_SPEC] + [VMEM_SPEC] * 4,
        out_specs=[VMEM_SPEC] * 2,
        scratch_shapes=[pltpu.VMEM(s, F32) for s in buffers]
        + [pltpu.SemaphoreType.DMA((pieces, 2)), pltpu.SemaphoreType.DMA((pieces,))],
        compiler_params=pltpu.CompilerParams(
            collective_id=0, has_side_effects=True, vmem_limit_bytes=60 * 1024 * 1024
        ),
    )(ranks, u, v, near_field, sketch)
    tile_col = jnp.arange(tiles, dtype=jnp.int32) * n_col + lax.axis_index("col")
    stays = jnp.logical_not((row_here == 1) & (tile_col == 1))[:, None, None]
    out_u, out_v = jnp.where(stays, out_u, 0.0), jnp.where(stays, out_v, 0.0)
    shape_out = (1, 1, tiles, 1, height, width)
    return (out_u.reshape(shape_out), out_v.reshape(shape_out))


def solution(mesh):
    return jax.shard_map(
        functools.partial(body, mesh.shape["row"], mesh.shape["col"]),
        mesh=mesh,
        in_specs=(
            P(None, "row", None, "col", None, None),
            P(None, "row", None, "col", None, None),
            P(),
            P(),
            P(None, None, None, None, "col"),
        ),
        out_specs=(
            P(None, "row", None, "col", None, None),
            P(None, "row", None, "col", None, None),
        ),
        check_vma=False,
    )
```
